32 devices in a mesh: px: 8 (over z, y), py: 4 (over x, core).
Axes of the slice: x: 2, y: 2, z: 4, core: 2. Of those that a mesh axis runs over, the one named last changes fastest.
Arguments:
- initial_field: float32 [1, 2048, 2048], P(None, ('px', 'py')), may hold values from -6 to 6
- target_field: float32 [1, 2048, 2048], P(None, ('px', 'py')), may hold values from -6 to 6
- forcing: float32 [2, 2048, 2048], P(None, ('px', 'py')), may hold values from -6 to 6
Outputs:
- next_field: float32 [1, 2048, 2048], P(None, ('px', 'py'))
- objective: float32 [], replicated
- field_grad: float32 [1, 2048, 2048], P(None, ('px', 'py'))
- forcing_grad: float32 [2, 2048, 2048], P(None, ('px', 'py'))
The draws below stay inside these ranges and needn't reach their ends.
All inputs are finite; a program needn't handle non-finite values.
Results may differ from the reference program's by a relative error of at most 0.00014.
Values sent between devices are 32-bit elements; how exact they have to be, the bound alone decides.
No kernel may reach another device: no remote copies, remote signals or barrier semaphores. Data moves between devices by JAX's collectives and lax.ppermute only.
A program may use at most 128 MiB of HBM per device.

```python
import jax
import jax.numpy as jnp
from jax import lax

NX = 2048
NY = 2048
MEMBERS = 1


def block_scale(own_key, dims, shards, low, largest):
    def one(dim, shards_of):
        heights = jax.random.uniform(jax.random.fold_in(jax.random.fold_in(own_key, 6), dim), (shards_of,), jnp.float32, low / len(shards), largest / len(shards))
        return jnp.repeat(jnp.exp(heights), dims[dim] // shards_of).reshape((-1,) + (1,) * (len(dims) - dim - 1))

    level = one(*shards[0])
    for cut in shards[1:]:
        level = level * one(*cut)
    return level


def gaussian(key, extent, deviation, bound, cuts=(), held_as=jnp.bfloat16):
    values = deviation * jax.random.normal(key, extent, jnp.float32)
    if cuts:
        values = values * block_scale(key, extent, cuts, -0.22, 0.18)
    return jnp.clip(values, -bound, bound).astype(held_as)


def setup_inputs(seed: int = 0) -> dict:
    arg_keys = jax.random.split(jax.random.key(seed), 4)
    initial_field = gaussian(arg_keys[0], (MEMBERS, NX, NY), 1.0, 6.0, ((1, 32),), jnp.float32)
    target_field = gaussian(arg_keys[1], (MEMBERS, NX, NY), 1.0, 6.0, ((1, 32),), jnp.float32)
    forcing = gaussian(arg_keys[2], (2, NY, NX), 1.0, 6.0, ((1, 32),), jnp.float32)
    return {"initial_field": initial_field, "target_field": target_field, "forcing": forcing}


time_step = 0.25

def wavenumbers(count):
    position = jnp.arange(count, dtype=jnp.int32)
    signed = jnp.where(position < count // 2, position, position - count)
    waves = (4.0 * signed.astype(jnp.float32) / count).astype(jnp.float32)
    derive = jnp.where(position == count // 2, jnp.float32(0.0), waves).astype(jnp.float32)
    return (waves, derive)

def advance(field, forcing):
    wave_first, deriv_first = wavenumbers(NX)
    wave_second, deriv_second = wavenumbers(NY)
    wave_square = wave_first[:, None] ** 2 + wave_second[None, :] ** 2
    denominator = 1.0 + time_step * (wave_square * wave_square - wave_square)
    state_hat = jnp.fft.fft2(field, norm='ortho')
    grad_first = jnp.fft.ifft2(1j * deriv_first[:, None] * state_hat, norm='ortho').real
    grad_second = jnp.fft.ifft2(1j * deriv_second[None, :] * state_hat, norm='ortho').real
    nonlinear = -0.5 * (grad_first * grad_first + grad_second * grad_second)
    nonlinear_hat = jnp.fft.fft2(nonlinear, norm='ortho')
    forcing_hat = lax.complex(forcing[0].T, forcing[1].T)
    next_hat = (state_hat + time_step * (nonlinear_hat + forcing_hat)) / denominator
    return jnp.fft.ifft2(next_hat, norm='ortho').real

def reference(initial_field, target_field, forcing):

    def one_member(pair):
        field, goal = pair
        next_one, pullback = jax.vjp(advance, field, forcing)
        residual = next_one - goal
        grad_one, forcing_one = pullback(residual)
        return (next_one, jnp.sum(residual * residual), grad_one, forcing_one)
    next_field, squares, field_grad, forcing_parts = lax.map(one_member, (initial_field, target_field))
    objective = 0.5 * jnp.sum(squares) / (MEMBERS * NX * NY)
    forcing_grad = lax.optimization_barrier(jnp.sum(forcing_parts, axis=0))
    return (next_field, objective, field_grad, forcing_grad)
```

```python
import math

import jax
import jax.numpy as jnp
import numpy as np
from jax import lax
from jax.experimental import pallas as pl
from jax.experimental.pallas import tpu as pltpu
from jax.sharding import PartitionSpec as P

time_step = 0.25
highest = lax.Precision.HIGHEST


def factor_pair(length):
    first_len = int(math.isqrt(length))
    while length % first_len:
        first_len -= 1
    return (first_len, length // first_len)


def phases(row_count, col_count, period, sign_value, factor):
    product = (
        jnp.arange(row_count, dtype=jnp.int32)[:, None]
        * jnp.arange(col_count, dtype=jnp.int32)[None, :]
        % period
    )
    angles = product.astype(jnp.float32) * (2.0 * math.pi / period)
    return (factor * jnp.cos(angles), sign_value * factor * jnp.sin(angles))


def complex_einsum(formula, left_real, left_imag, table_pair):
    real_term = jnp.einsum(formula, left_real, table_pair[0], precision=highest)
    imag_term = jnp.einsum(formula, left_real, table_pair[1], precision=highest)
    if left_imag is None:
        return (real_term, imag_term)
    real_term = real_term - jnp.einsum(formula, left_imag, table_pair[1], precision=highest)
    imag_term = imag_term + jnp.einsum(formula, left_imag, table_pair[0], precision=highest)
    return (real_term, imag_term)


def transform(real_part, imag_part, sign_value, leading, real_only):
    if leading:
        members, length, span_rows = real_part.shape
        first_len, second_len = factor_pair(length)
        new_shape = (members, first_len, second_len, span_rows)
        formula = "mabr,ak->mrkb"
    else:
        members, span_rows, length = real_part.shape
        first_len, second_len = factor_pair(length)
        new_shape = (members, span_rows, first_len, second_len)
        formula = "mrab,ak->mrkb"
    shaped_real = real_part.reshape(new_shape)
    shaped_imag = None if imag_part is None else imag_part.reshape(new_shape)
    sectioned_out = complex_einsum(
        formula, shaped_real, shaped_imag, phases(first_len, first_len, first_len, sign_value, 1.0)
    )
    twiddle = phases(first_len, second_len, length, sign_value, 1.0 / math.sqrt(length))
    turned_real = sectioned_out[0] * twiddle[0] - sectioned_out[1] * twiddle[1]
    turned_imag = sectioned_out[0] * twiddle[1] + sectioned_out[1] * twiddle[0]
    last_table = phases(second_len, second_len, second_len, sign_value, 1.0)
    final_formula = "mrkb,bq->mrqk"
    if real_only:
        out_real = jnp.einsum(final_formula, turned_real, last_table[0], precision=highest)
        out_real = out_real - jnp.einsum(
            final_formula, turned_imag, last_table[1], precision=highest
        )
        return (out_real.reshape(members, span_rows, length), None)
    out_real, out_imag = complex_einsum(final_formula, turned_real, turned_imag, last_table)
    return (
        out_real.reshape(members, span_rows, length),
        out_imag.reshape(members, span_rows, length),
    )


def regroup(real_part, imag_part):
    moved_real, moved_imag = (
        lax.all_to_all(real_part, ("px", "py"), split_axis=2, concat_axis=1, tiled=True),
        lax.all_to_all(imag_part, ("px", "py"), split_axis=2, concat_axis=1, tiled=True),
    )
    return (moved_real, moved_imag)


def spectral(real_part, imag_part):
    first_pass = transform(real_part, imag_part, -1.0, False, False)
    moved = regroup(first_pass[0], first_pass[1])
    return transform(moved[0], moved[1], -1.0, True, False)


def physical(real_part, imag_part, real_only):
    first_pass = transform(real_part, imag_part, 1.0, False, False)
    moved = regroup(first_pass[0], first_pass[1])
    return transform(moved[0], moved[1], 1.0, True, real_only)


def waves_of(position, count):
    signed = jnp.where(position < count // 2, position, position - count)
    waves = 4.0 * signed.astype(jnp.float32) / count
    derive = jnp.where(position == count // 2, jnp.float32(0.0), waves)
    return (waves, derive)


def per_device_plain(initial_field, target_field, forcing):
    members = initial_field.shape[0]
    full_second = initial_field.shape[2]
    spec_rows = forcing.shape[1]
    full_first = forcing.shape[2]
    device = lax.axis_index(("px", "py"))
    position_first = jnp.arange(full_first, dtype=jnp.int32)
    position_second = device * spec_rows + jnp.arange(spec_rows, dtype=jnp.int32)
    wave_first, deriv_first = waves_of(position_first, full_first)
    wave_second, deriv_second = waves_of(position_second, full_second)
    wave_first = wave_first[None, :]
    deriv_first = deriv_first[None, :]
    wave_second = wave_second[:, None]
    deriv_second = deriv_second[:, None]
    wave_square = wave_first * wave_first + wave_second * wave_second
    denominator = 1.0 + time_step * (wave_square * wave_square - wave_square)
    state_real, state_imag = spectral(initial_field, None)
    slope_real = -deriv_first * state_imag - deriv_second * state_real
    slope_imag = deriv_first * state_real - deriv_second * state_imag
    grad_first, grad_second = physical(slope_real, slope_imag, False)
    nonlinear = -0.5 * (grad_first * grad_first + grad_second * grad_second)
    nonlinear_real, nonlinear_imag = spectral(nonlinear, None)
    next_real = (state_real + time_step * (nonlinear_real + forcing[0])) / denominator
    next_imag = (state_imag + time_step * (nonlinear_imag + forcing[1])) / denominator
    next_field, unused_part = physical(next_real, next_imag, True)
    residual = next_field - target_field
    total = lax.psum(0.5 * jnp.sum(residual * residual), ("px", "py"))
    objective = total / (members * full_first * full_second)
    misfit_real, misfit_imag = spectral(residual, None)
    coef_real = misfit_real / denominator
    coef_imag = misfit_imag / denominator
    forcing_grad = time_step * jnp.stack([jnp.sum(coef_real, axis=0), jnp.sum(coef_imag, axis=0)])
    multiplier, unused_other = physical(time_step * coef_real, time_step * coef_imag, True)
    joint_real, joint_imag = spectral(multiplier * grad_first, multiplier * grad_second)
    total_real = coef_real - deriv_first * joint_imag + deriv_second * joint_real
    total_imag = coef_imag + deriv_first * joint_real + deriv_second * joint_imag
    field_grad, unused_last = physical(total_real, total_imag, True)
    return (next_field, objective, field_grad, forcing_grad)


def split_of(value):
    high = value.astype(jnp.bfloat16)
    low = (value - high.astype(jnp.float32)).astype(jnp.bfloat16)
    return high, low


def dots(high, low, table_high, table_low):
    def one(left, right):
        return jnp.dot(left, right, preferred_element_type=jnp.float32)

    return one(high, table_high) + (one(low, table_high) + one(high, table_low))


def turn(pair, cosine, sine):
    real, imag = pair
    return real * cosine - imag * sine, imag * cosine + real * sine


def butterflies(values, sign):
    count = len(values)
    if count == 1:
        return values
    even = butterflies(values[0::2], sign)
    odd = butterflies(values[1::2], sign)
    half = count // 2
    first, second = [], []
    root = math.sqrt(0.5)
    for place in range(half):
        real, imag = odd[place]
        if place == 0:
            turned = (real, imag)
        elif 4 * place == count:
            turned = (-sign * imag, sign * real)
        elif 8 * place == count:
            turned = (root * (real - sign * imag), root * (imag + sign * real))
        elif 8 * place == 3 * count:
            turned = (root * (-real - sign * imag), root * (sign * real - imag))
        else:
            angle = 2.0 * math.pi * place / count
            turned = turn((real, imag), math.cos(angle), sign * math.sin(angle))
        base_real, base_imag = even[place]
        first.append((base_real + turned[0], base_imag + turned[1]))
        second.append((base_real - turned[0], base_imag - turned[1]))
    return first + second


def np_split(table):
    high = np.asarray(table, np.float32).astype(jnp.bfloat16)
    low = (np.asarray(table, np.float64) - high.astype(np.float64)).astype(jnp.bfloat16)
    return jnp.asarray(high), jnp.asarray(low)


class Tables:
    def __init__(self, length, parts):
        radix = 8
        inner = length // radix
        lanes = length // parts
        scale = 1.0 / math.sqrt(length)
        spot = np.arange(inner)
        angle = 2.0 * np.pi * (np.outer(spot, spot) % inner) / inner
        self.row_pair = np_split(scale * np.concatenate([np.cos(angle), np.sin(angle)], 1))
        classes = np.arange(radix)
        angle = 2.0 * np.pi * np.outer(classes, spot) / length
        self.row_turn = (
            jnp.asarray(np.cos(angle), jnp.float32),
            jnp.asarray(np.sin(angle), jnp.float32),
        )
        half = inner // 2
        front = np.arange(half)
        angle = 2.0 * np.pi * (np.outer(front, spot) % inner) / inner
        real_rows, imag_rows = 2.0 * np.cos(angle), -2.0 * np.sin(angle)
        real_rows[0] = 1.0
        imag_rows[0] = np.where(spot % 2 == 0, 1.0, -1.0)
        self.even_pair = np_split(scale * np.concatenate([real_rows, imag_rows], 0))
        angle = 2.0 * np.pi * (np.outer(4 + radix * (front + half), spot) % length) / length
        self.odd_pair = np_split(
            scale * np.concatenate([2.0 * np.cos(angle), -2.0 * np.sin(angle)], 0)
        )
        place = np.arange(lanes)
        angle = 2.0 * np.pi * (np.outer(place, place) % lanes) / lanes
        eye = np.eye(inner // lanes)
        self.col_pair = np_split(
            scale * np.concatenate([np.kron(eye, np.cos(angle)), np.kron(eye, np.sin(angle))], 1)
        )
        outer = np.arange(parts)
        angle = 2.0 * np.pi * np.outer(outer, np.tile(place, inner // lanes)) / length
        self.col_turn = (
            jnp.asarray(np.cos(angle), jnp.float32),
            jnp.asarray(np.sin(angle), jnp.float32),
        )
        index = outer[:, None] + parts * np.tile(place, inner // lanes)[None, :]
        signed = np.where(index < length // 2, index, index - length)
        waves = 4.0 * signed / length
        self.col_wave = waves
        self.col_deriv = jnp.asarray(np.where(index == length // 2, 0.0, waves), jnp.float32)
        index = np.stack([radix * spot + one for one in range(4)])
        index[0, half:] += 4
        signed = np.where(index < length // 2, index, index - length)
        waves = 4.0 * signed / length
        waves[0, 0] = 0.0
        self.row_deriv = jnp.asarray(waves, jnp.float32)


def eight_real(blocks):
    plus = [blocks[i] + blocks[i + 4] for i in range(4)]
    minus = [blocks[i] - blocks[i + 4] for i in range(4)]
    root = math.sqrt(0.5)
    even, odd = plus[0] + plus[2], plus[1] + plus[3]
    near, far = root * (minus[1] - minus[3]), root * (minus[1] + minus[3])
    return {
        0: even + odd,
        4: even - odd,
        1: (minus[0] + near, -minus[2] - far),
        2: (plus[0] - plus[2], plus[3] - plus[1]),
        3: (minus[0] - near, minus[2] - far),
    }


def rows_forward(load, high, low, product, pair, spin, other):
    for row in range(0, 64, 16):
        for lane in range(0, 256, 128):
            rows, lanes = slice(row, row + 16), slice(lane, lane + 128)
            mixed = eight_real([load(one, rows, lanes) for one in range(8)])

            def spun(kind, real, imag):
                cosine = spin[0][kind : kind + 1, lanes]
                sine = spin[1][kind : kind + 1, lanes]
                if imag is None:
                    return real * cosine, -real * sine
                return real * cosine + imag * sine, imag * cosine - real * sine

            out = [None] * 9
            out[0] = mixed[0]
            for one in (1, 2, 3):
                if other:
                    real, imag = mixed[4 - one]
                    out[one], out[3 + one] = spun(4 + one, real, -imag)
                else:
                    out[one], out[3 + one] = spun(one, *mixed[one])
            out[7], out[8] = spun(4, mixed[4], None)
            for place in range(9):
                top, bottom = split_of(out[place])
                at = slice(64 * place + row, 64 * place + row + 16)
                high[at, lanes] = top
                low[at, lanes] = bottom
    product[0:576, :] = dots(high[0:576, :], low[0:576, :], pair[0][...], pair[1][...])

    def cosine(place, lanes=slice(0, 256)):
        return product[64 * place : 64 * place + 64, lanes]

    def sine(place, lanes=slice(0, 256)):
        moved = slice(lanes.start + 256, lanes.stop + 256)
        return product[64 * place : 64 * place + 64, moved]

    front, back = slice(0, 128), slice(128, 256)
    if other:
        real = [jnp.concatenate([cosine(7, front) + sine(8, front), cosine(0, back)], 1)]
        imag = [jnp.concatenate([cosine(8, front) - sine(7, front), -sine(0, back)], 1)]
    else:
        lane = lax.broadcasted_iota(jnp.int32, (64, 128), 1)
        first = jnp.where(lane == 0, cosine(0, back), -sine(0, front))
        real = [jnp.concatenate([cosine(0, front), cosine(7, back) + sine(8, back)], 1)]
        imag = [jnp.concatenate([first, cosine(8, back) - sine(7, back)], 1)]
    for one in (1, 2, 3):
        real.append(cosine(one) + sine(3 + one))
        imag.append(cosine(3 + one) - sine(one))
    return real + imag


def rows_store(slots, target, offset):
    for place in range(0, 8, 2):
        both = jnp.concatenate([slots[place], slots[place + 1]], 0)
        target[:, :, offset + 64 * place : offset + 64 * place + 128] = both.T.reshape(32, 8, 128)


def rows_derived(slots, deriv):
    out = [None] * 8
    for one in range(4):
        wave = deriv[one : one + 1, :]
        out[one] = -wave * slots[4 + one]
        out[4 + one] = wave * slots[one]
    return out


def rows_loaded(source, offset):
    out = []
    for place in range(0, 8, 2):
        both = source[:, :, offset + 64 * place : offset + 64 * place + 128]
        both = both.reshape(256, 128).T
        out += [both[:64], both[64:]]
    return out


def put(high, low, place, value):
    top, bottom = split_of(value)
    high[64 * place : 64 * place + 64, :] = top
    low[64 * place : 64 * place + 64, :] = bottom


def eight_inverse(even, odd, ones, twos, threes, store):
    root = math.sqrt(0.5)
    plus, minus = even + odd, even - odd
    back = root * (ones[0] - ones[1]) - root * (threes[0] + threes[1])
    fore = root * (threes[0] - threes[1]) - root * (ones[0] + ones[1])
    parts = (
        (plus + twos[0], ones[0] + threes[0]),
        (minus - twos[1], back),
        (plus - twos[0], threes[1] - ones[1]),
        (minus + twos[1], fore),
    )
    for one in range(4):
        store(one, parts[one][0] + parts[one][1])
        store(one + 4, parts[one][0] - parts[one][1])


def rows_inverse(slots, high, low, product, pair, even, odd, spin, store):
    for one in (1, 2, 3):
        put(high, low, one - 1, slots[one])
        put(high, low, 2 + one, slots[4 + one])
    front, back = slice(0, 128), slice(128, 256)
    put(high, low, 6, jnp.concatenate([slots[0][:, front], slots[4][:, front]], 1))
    put(high, low, 7, jnp.concatenate([slots[0][:, back], slots[4][:, back]], 1))
    product[0:384, :] = dots(high[0:384, :], low[0:384, :], pair[0][...], pair[1][...])
    product[384:448, 0:256] = dots(high[384:448, :], low[384:448, :], even[0][...], even[1][...])
    product[384:448, 256:512] = dots(high[448:512, :], low[448:512, :], odd[0][...], odd[1][...])
    for row in range(0, 64, 16):
        for lane in range(0, 256, 128):
            turned = []
            for one in (1, 2, 3):
                at = slice(64 * (one - 1) + row, 64 * (one - 1) + row + 16)
                to = slice(64 * (2 + one) + row, 64 * (2 + one) + row + 16)
                lanes, moved = slice(lane, lane + 128), slice(lane + 256, lane + 384)
                value = (
                    product[at, lanes] - product[to, moved],
                    product[to, lanes] + product[at, moved],
                )
                value = turn(
                    value,
                    2.0 * spin[0][one : one + 1, lanes],
                    2.0 * spin[1][one : one + 1, lanes],
                )
                turned.append(value)
            at = slice(384 + row, 400 + row)
            eight_inverse(
                product[at, lane : lane + 128],
                product[at, lane + 256 : lane + 384],
                *turned,
                lambda one, value: store(one, slice(row, row + 16), slice(lane, lane + 128), value),
            )


def rows_whole(source, offset, high, low, product, pair, spin, store):
    for place in range(0, 16, 2):
        both = source[:, :, offset + 64 * place : offset + 64 * place + 128]
        both = both.reshape(256, 128).T
        top, bottom = split_of(both)
        high[64 * place : 64 * place + 128, :] = top
        low[64 * place : 64 * place + 128, :] = bottom
    product[...] = dots(high[...], low[...], pair[0][...], pair[1][...])
    for row in range(0, 64, 16):
        for lane in range(0, 256, 128):
            lanes, moved = slice(lane, lane + 128), slice(lane + 256, lane + 384)
            turned = []
            for one in range(8):
                at = slice(64 * one + row, 64 * one + row + 16)
                to = slice(512 + 64 * one + row, 512 + 64 * one + row + 16)
                value = (
                    product[at, lanes] - product[to, moved],
                    product[to, lanes] + product[at, moved],
                )
                turned.append(
                    turn(value, spin[0][one : one + 1, lanes], spin[1][one : one + 1, lanes])
                )
            joint = [
                (turned[one][0] + turned[8 - one][0], turned[one][1] - turned[8 - one][1])
                for one in (1, 2, 3)
            ]
            eight_inverse(
                turned[0][0],
                turned[4][0],
                *joint,
                lambda one, value: store(one, slice(row, row + 16), slice(lane, lane + 128), value),
            )


def put_tiles(high, low, place, first, second, lanes):
    top, bottom = split_of(jnp.concatenate([first, second], 0))
    high[8 * place : 8 * place + 16, lanes] = top
    low[8 * place : 8 * place + 16, lanes] = bottom


def cols_forward(source, offset, high, low, product, pair, spin):
    for lane in range(0, 256, 128):
        lanes = slice(lane, lane + 128)
        values = [
            (
                source[one, :, offset + lane : offset + lane + 128],
                source[one, :, offset + 256 + lane : offset + 384 + lane],
            )
            for one in range(32)
        ]
        values = butterflies(values, -1)
        for one in range(32):
            values[one] = turn(
                values[one], spin[0][one : one + 1, lanes], -spin[1][one : one + 1, lanes]
            )
        for one in range(0, 32, 2):
            put_tiles(high, low, one, values[one][0], values[one + 1][0], lanes)
            put_tiles(high, low, 32 + one, values[one][1], values[one + 1][1], lanes)
    product[0:512, :] = dots(high[0:512, :], low[0:512, :], pair[0][...], pair[1][...])

    def tile(one, lanes=slice(0, 256)):
        at, to = slice(8 * one, 8 * one + 8), slice(256 + 8 * one, 264 + 8 * one)
        moved = slice(lanes.start + 256, lanes.stop + 256)
        return (
            product[at, lanes] + product[to, moved],
            product[to, lanes] - product[at, moved],
        )

    return tile


def cols_inverse(tile, high, low, product, pair, spin, target, offset, count=1):
    for group in range(count):
        for one in range(0, 32, 2):
            first, second = tile(one, group), tile(one + 1, group)
            put_tiles(high, low, one, first[0], second[0], slice(0, 256))
            put_tiles(high, low, 32 + one, first[1], second[1], slice(0, 256))
        product[0:512, :] = dots(high[0:512, :], low[0:512, :], pair[0][...], pair[1][...])
        for lane in range(0, 256, 128):
            lanes, moved = slice(lane, lane + 128), slice(lane + 256, lane + 384)
            values = []
            for one in range(32):
                at, to = slice(8 * one, 8 * one + 8), slice(256 + 8 * one, 264 + 8 * one)
                value = (
                    product[at, lanes] - product[to, moved],
                    product[to, lanes] + product[at, moved],
                )
                values.append(
                    turn(value, spin[0][one : one + 1, lanes], spin[1][one : one + 1, lanes])
                )
            values = butterflies(values, 1)
            for one in range(32):
                at = offset + 256 * group + lane
                target[one, :, at : at + 128] = values[one][0]
                at += 256 * count
                target[one, :, at : at + 128] = values[one][1]


def mirrored(tile, one):
    real, imag = tile((32 - one) % 32)
    lane = lax.broadcasted_iota(jnp.int32, (8, 128), 1)
    spot = jnp.where(lane < 64, (64 - lane) % 64 if one == 0 else 63 - lane, lane)
    return (
        jnp.take_along_axis(real, spot, axis=1),
        -jnp.take_along_axis(imag, spot, axis=1),
    )


def kernel_start(field, ph, pl_, sc, ss, out, high, low, product):
    def load(one, rows, lanes):
        return field[rows, 256 * one + lanes.start : 256 * one + lanes.stop]

    slots = rows_forward(load, high, low, product, (ph, pl_), (sc, ss), False)
    rows_store(slots, out, 0)


def kernel_slope(field, ph, pl_, eh, el, oh, ol, sc, ss, deriv, out, high, low, product):
    def load(one, rows, lanes):
        return field[rows, 256 * one + lanes.start : 256 * one + lanes.stop]

    def store(one, rows, lanes, value):
        out[rows, 256 * one + lanes.start : 256 * one + lanes.stop] = value

    slots = rows_forward(load, high, low, product, (ph, pl_), (sc, ss), False)
    slots = rows_derived(slots, deriv)
    rows_inverse(
        slots, high, low, product, (ph, pl_), (eh, el), (oh, ol), (sc, ss), store
    )


def kernel_force(force, ch, cl, tc, ts, out, mixed, turned, spec, high, low, product):
    for lane in range(0, 2048, 128):
        both = jnp.concatenate([force[part, :, lane : lane + 128] for part in range(2)], 0)
        turned[lane : lane + 128, :] = both.T
    lane = lax.broadcasted_iota(jnp.int32, (8, 128), 1)
    for one in range(0, 32, 2):
        both = jnp.concatenate(
            [turned[pl.ds(one, 64, stride=32), :], turned[pl.ds(one + 1, 64, stride=32), :]], 0
        ).T
        base = 64 * one
        mixed[base : base + 128, :] = both
        for part in range(2):
            for kind in range(0, 8, 2):
                at = base + 64 * part + kind
                first = mixed[pl.ds(at, 8, stride=8), :]
                second = mixed[pl.ds(at + 1, 8, stride=8), :]
                lanes = slice(512 * part + 64 * kind, 512 * part + 64 * kind + 128)
                spec[8 * one : 8 * one + 8, lanes] = jnp.where(
                    lane < 64, first, pltpu.roll(second, 64, 1)
                )
                spec[8 * one + 8 : 8 * one + 16, lanes] = jnp.where(
                    lane < 64, pltpu.roll(first, 64, 1), second
                )

    def tile(one, group):
        rows = slice(8 * one, 8 * one + 8)
        return (
            spec[rows, 256 * group : 256 * group + 256],
            spec[rows, 512 + 256 * group : 768 + 256 * group],
        )

    cols_inverse(tile, high, low, product, (ch, cl), (tc, ts), out, 0, 2)


def kernel_first(source, other, ch, cl, tc, ts, deriv, state, out, high, low, product):
    tile = cols_forward(source, 0, high, low, product, (ch, cl), (tc, ts))
    for one in range(32):
        rows = slice(8 * one, 8 * one + 8)
        real, imag = tile(one)
        state[0, rows, :] = real
        state[1, rows, :] = imag

    def slope(one, group):
        rows = slice(8 * one, 8 * one + 8)
        wave = deriv[one : one + 1, :]
        return -wave * state[1, rows, :], wave * state[0, rows, :]

    cols_inverse(slope, high, low, product, (ch, cl), (tc, ts), out, 0)
    out[:, :, 512:1536] = other[...]


def kernel_bend(
    source, second, other, ph, pl_, eh, el, oh, ol, sc, ss, grad, out, bend, high, low, product
):
    def put_bend(one, rows, lanes, value):
        bend[rows, 256 * one + lanes.start : 256 * one + lanes.stop] = value

    rows_whole(source, 512, high, low, product, (ph, pl_), (sc, ss), put_bend)

    def store(one, rows, lanes, value):
        to = slice(256 * one + lanes.start, 256 * one + lanes.stop)
        grad[rows, to] = value
        side = second[rows, to]
        bend[rows, to] = bend[rows, to] - 0.5 * (value * value + side * side)

    slots = rows_loaded(source, 0)
    rows_inverse(slots, high, low, product, (ph, pl_), (eh, el), (oh, ol), (sc, ss), store)

    def load(one, rows, lanes):
        return bend[rows, 256 * one + lanes.start : 256 * one + lanes.stop]

    slots = rows_forward(load, high, low, product, (ph, pl_), (sc, ss), False)
    rows_store(slots, out, 0)
    out[:, :, 512:1024] = other[...]


def kernel_solve(
    source, state, damp, cross, ch, cl, tc, ts, coef, out, goal, fresh, high, low, product
):
    tile = cols_forward(source, 512, high, low, product, (ch, cl), (tc, ts))
    for one in range(32):
        rows = slice(8 * one, 8 * one + 8)
        goal[0, rows, :], goal[1, rows, :] = tile(one)
    tile = cols_forward(source, 0, high, low, product, (ch, cl), (tc, ts))
    for one in range(32):
        rows = slice(8 * one, 8 * one + 8)
        real, imag = tile(one)
        fresh[0, rows, :] = state[0, rows, :] + time_step * real
        fresh[1, rows, :] = state[1, rows, :] + time_step * imag

    def front(array):
        def view(one):
            rows = slice(8 * one, 8 * one + 8)
            return array[0, rows, 0:128], array[1, rows, 0:128]

        return view

    def damped(value, flipped, one):
        rows = slice(8 * one, 8 * one + 8)
        weight, mixed = damp[rows, :], cross[rows, :]
        return tuple(
            jnp.concatenate(
                [
                    value[part][:, 0:128] * weight[:, 0:128] + flipped[part] * mixed,
                    value[part][:, 128:256] * weight[:, 128:256],
                ],
                1,
            )
            for part in range(2)
        )

    held = []
    for one in range(32):
        rows = slice(8 * one, 8 * one + 8)
        value = (fresh[0, rows, :], fresh[1, rows, :])
        flipped = mirrored(front(fresh), one)
        following = damped(value, flipped, one)
        weight, mixed = damp[rows, 0:128], cross[rows, :]
        back = mirrored(front(goal), one)
        turned_back = tuple(
            flipped[part] * weight + value[part][:, 0:128] * mixed - back[part]
            for part in range(2)
        )
        miss = tuple(following[part] - goal[part, rows, :] for part in range(2))
        slope = damped(miss, turned_back, one)
        for part in range(2):
            coef[part, rows, :] = time_step * slope[part]
            goal_next = following[part]
            product[256 * part + 8 * one : 256 * part + 8 * one + 8, 0:256] = goal_next
    for part in range(2):
        fresh[part, :, :] = product[256 * part : 256 * part + 256, 0:256]

    def scaled(one, group):
        rows = slice(8 * one, 8 * one + 8)
        return coef[0, rows, :], coef[1, rows, :]

    def following_tile(one, group):
        rows = slice(8 * one, 8 * one + 8)
        return fresh[0, rows, :], fresh[1, rows, :]

    cols_inverse(scaled, high, low, product, (ch, cl), (tc, ts), out, 0)
    cols_inverse(following_tile, high, low, product, (ch, cl), (tc, ts), out, 512)


def kernel_adjoint(
    source, grad, ph, pl_, eh, el, oh, ol, sc, ss, mult, out, joint, high, low, product
):
    def store(one, rows, lanes, value):
        to = slice(256 * one + lanes.start, 256 * one + lanes.stop)
        mult[rows, to] = value
        joint[rows, to] = value * grad[rows, to]

    slots = rows_loaded(source, 0)
    rows_inverse(slots, high, low, product, (ph, pl_), (eh, el), (oh, ol), (sc, ss), store)

    def load(one, rows, lanes):
        return joint[rows, 256 * one + lanes.start : 256 * one + lanes.stop]

    slots = rows_forward(load, high, low, product, (ph, pl_), (sc, ss), False)
    rows_store(slots, out, 0)

    def load_other(one, rows, lanes):
        return mult[rows, 256 * one + lanes.start : 256 * one + lanes.stop]

    slots = rows_forward(load_other, high, low, product, (ph, pl_), (sc, ss), True)
    rows_store(slots, out, 512)


def kernel_side(
    source, goal, mult, second, ph, pl_, eh, el, oh, ol, sc, ss, deriv,
    ahead, side, miss, joint, high, low, product,
):
    def store(one, rows, lanes, value):
        to = slice(256 * one + lanes.start, 256 * one + lanes.stop)
        ahead[rows, to] = value
        joint[rows, to] = mult[rows, to] * second[rows, to]

    slots = rows_loaded(source, 512)
    rows_inverse(slots, high, low, product, (ph, pl_), (eh, el), (oh, ol), (sc, ss), store)
    total = jnp.zeros((8, 256), jnp.float32)
    for row in range(0, 64, 8):
        for lane in range(0, 2048, 256):
            gap = ahead[row : row + 8, lane : lane + 256] - goal[row : row + 8, lane : lane + 256]
            total = total + gap * gap
    miss[...] = jnp.broadcast_to(0.5 * jnp.sum(total), (8, 128))

    def load(one, rows, lanes):
        return joint[rows, 256 * one + lanes.start : 256 * one + lanes.stop]

    slots = rows_forward(load, high, low, product, (ph, pl_), (sc, ss), False)
    slots = rows_derived(slots, deriv)
    for place in range(8):
        side[64 * place : 64 * place + 64, :] = slots[place]


def kernel_last(source, coef, miss, ch, cl, tc, ts, deriv, out, spec, high, low, product):
    tile = cols_forward(source, 0, high, low, product, (ch, cl), (tc, ts))
    for one in range(32):
        rows = slice(8 * one, 8 * one + 8)
        real, imag = tile(one)
        wave = deriv[one : one + 1, :]
        spec[0, rows, :] = coef[0, rows, :] * (1.0 / time_step) - wave * imag
        spec[1, rows, :] = coef[1, rows, :] * (1.0 / time_step) + wave * real

    def whole(one, group):
        rows = slice(8 * one, 8 * one + 8)
        return spec[0, rows, :], spec[1, rows, :]

    cols_inverse(whole, high, low, product, (ch, cl), (tc, ts), out, 0)
    out[:, :, 512:640] = jnp.broadcast_to(miss[...][None], (32, 8, 128))


def kernel_force_grad(
    place, source, coef, ch, cl, tc, ts, out, mixed, turned, high, low, product
):
    tile = cols_forward(source, 512, high, low, product, (ch, cl), (tc, ts))
    early = place[0] < 16
    corner = place[0] == 0
    lane = lax.broadcasted_iota(jnp.int32, (8, 128), 1)
    row = lax.broadcasted_iota(jnp.int32, (8, 128), 0)
    packed = jnp.logical_and(jnp.logical_and(row == 0, lane < 64), corner)

    def front(one):
        rows = slice(8 * one, 8 * one + 8)
        return coef[0, rows, 0:128], coef[1, rows, 0:128]

    def lanes_of(one):
        rows = slice(8 * one, 8 * one + 8)
        far = tile(one)
        flipped = mirrored(front, one)
        out_parts = []
        for part in range(2):
            near_front = coef[part, rows, 0:128]
            near_front = jnp.where(packed, 0.5 * (near_front + flipped[part]), near_front)
            near_back = coef[part, rows, 128:256]
            far_front, far_back = far[part][:, 0:128], far[part][:, 128:256]
            low_half = lane < 64
            swap = jnp.logical_and(low_half, jnp.logical_not(early))
            out_parts.append(
                [
                    jnp.where(swap, far_front, near_front),
                    near_back,
                    jnp.where(swap, near_front, far_front),
                    far_back,
                ]
            )
        return out_parts

    for one in range(0, 32, 2):
        first, second = lanes_of(one), lanes_of(one + 1)
        base = 64 * one
        for part in range(2):
            for pairs in range(4):
                left, right = first[part][pairs], second[part][pairs]
                at = base + 64 * part + 2 * pairs
                mixed[pl.ds(at, 8, stride=8), :] = jnp.where(
                    lane < 64, left, pltpu.roll(right, 64, 1)
                )
                mixed[pl.ds(at + 1, 8, stride=8), :] = jnp.where(
                    lane < 64, pltpu.roll(left, 64, 1), right
                )
        both = mixed[base : base + 128, :].T
        turned[pl.ds(one, 64, stride=32), :] = both[:64]
        turned[pl.ds(one + 1, 64, stride=32), :] = both[64:]
    for start in range(0, 2048, 128):
        both = turned[start : start + 128, :].T
        for part in range(2):
            out[part, :, start : start + 128] = both[64 * part : 64 * part + 64]


def kernel_finish(source, side, ph, pl_, eh, el, oh, ol, sc, ss, out, total, high, low, product):
    slots = rows_loaded(source, 0)
    slots = [slots[place] + side[64 * place : 64 * place + 64, :] for place in range(8)]

    def store(one, rows, lanes, value):
        out[rows, 256 * one + lanes.start : 256 * one + lanes.stop] = value

    rows_inverse(slots, high, low, product, (ph, pl_), (eh, el), (oh, ol), (sc, ss), store)
    total[...] = jnp.sum(source[:, :, 512:640], axis=0)


def call(body, outputs, scratch, *operands, scalars=0):
    specs = [pl.BlockSpec(memory_space=pltpu.SMEM)] * scalars
    specs += [pl.BlockSpec(memory_space=pltpu.VMEM)] * (len(operands) - scalars)
    return pl.pallas_call(
        body,
        out_shape=tuple(jax.ShapeDtypeStruct(one, jnp.float32) for one in outputs),
        in_specs=specs,
        out_specs=tuple(pl.BlockSpec(memory_space=pltpu.VMEM) for _ in outputs),
        scratch_shapes=scratch,
        name=body.__name__,
        compiler_params=pltpu.CompilerParams(vmem_limit_bytes=48 * 2**20),
    )(*operands)


def work(rows):
    return [
        pltpu.VMEM((rows, 256), jnp.bfloat16),
        pltpu.VMEM((rows, 256), jnp.bfloat16),
        pltpu.VMEM((rows, 512), jnp.float32),
    ]


def exchange(value):
    return lax.all_to_all(value, ("px", "py"), split_axis=0, concat_axis=0, tiled=True)


def per_device_fast(initial_field, target_field, forcing):
    length = initial_field.shape[2]
    local = initial_field.shape[1]
    parts = length // local
    device = lax.axis_index(("px", "py"))
    tables = Tables(length, parts)
    inner = length // 8
    field, goal = initial_field[0], target_field[0]
    rows_all = tables.row_pair + tables.even_pair + tables.odd_pair + tables.row_turn
    rows_some = tables.row_pair + tables.row_turn
    cols = tables.col_pair + tables.col_turn
    f32 = jnp.float32
    own = jnp.arange(8, dtype=jnp.int32)[None, :, None]
    kind = jnp.arange(inner, dtype=jnp.int32)[None, None, :] // local
    late = jnp.where(device < parts // 2, 0, 4)
    second = device * local + 8 * own + jnp.where(kind == 0, late, kind)
    wave_first = jnp.asarray(tables.col_wave, f32)[:, None, :]

    def inverse_of(index):
        wave = waves_of(index, length)[0]
        square = wave_first * wave_first + wave * wave
        return 1.0 / (1.0 + time_step * (square * square - square))

    packed = (second == 0) & (kind == 0)
    plain = inverse_of(second)
    middle = inverse_of(second + length // 2)
    damp = jnp.where(packed, 0.5 * (plain + middle), plain).reshape(inner, inner)
    cross = jnp.where(packed, 0.5 * (plain - middle), 0.0).reshape(inner, inner)[:, :128]

    block = (parts, 8, 512)
    (sent,) = call(kernel_start, [block], work(576), field, *rows_some)
    first = exchange(sent)
    (force,) = call(
        kernel_force,
        [(parts, 8, 1024)],
        [pltpu.VMEM((length, 128), f32), pltpu.VMEM((length, 128), f32), pltpu.VMEM((256, 1024), f32)]
        + work(512),
        forcing,
        *cols,
    )
    (goal_rows,) = call(kernel_start, [block], work(576), goal, *rows_some)
    (grad_second,) = call(
        kernel_slope, [(local, length)], work(576), field, *rows_all, tables.row_deriv
    )
    state, sent = call(
        kernel_first,
        [(2, 256, 256), (parts, 8, 1536)],
        work(512),
        first,
        force,
        *cols,
        tables.col_deriv,
    )
    moved = exchange(sent)
    grad_first, sent = call(
        kernel_bend,
        [(local, length), (parts, 8, 1024)],
        [pltpu.VMEM((local, length), f32)] + work(1024),
        moved,
        grad_second,
        goal_rows,
        *rows_all,
    )
    moved = exchange(sent)
    coef, sent = call(
        kernel_solve,
        [(2, 256, 256), (parts, 8, 1024)],
        [pltpu.VMEM((2, 256, 256), f32), pltpu.VMEM((2, 256, 256), f32)] + work(512),
        moved,
        state,
        damp,
        cross,
        *cols,
    )
    moved = exchange(sent)
    mult, sent = call(
        kernel_adjoint,
        [(local, length), (parts, 8, 1024)],
        [pltpu.VMEM((local, length), f32)] + work(576),
        moved,
        grad_first,
        *rows_all,
    )
    next_field, side, miss = call(
        kernel_side,
        [(local, length), (512, 256), (8, 128)],
        [pltpu.VMEM((local, length), f32)] + work(576),
        moved,
        goal,
        mult,
        grad_second,
        *rows_all,
        tables.row_deriv,
    )
    moved = exchange(sent)
    (sent,) = call(
        kernel_last,
        [(parts, 8, 640)],
        [pltpu.VMEM((2, 256, 256), f32)] + work(512),
        moved,
        coef,
        miss,
        *cols,
        tables.col_deriv,
    )
    (forcing_grad,) = call(
        kernel_force_grad,
        [(2, local, length)],
        [pltpu.VMEM((length, 128), f32), pltpu.VMEM((length, 128), f32)] + work(512),
        jnp.asarray(device, jnp.int32).reshape(1),
        moved,
        coef,
        *cols,
        scalars=1,
    )
    moved = exchange(sent)
    field_grad, total = call(
        kernel_finish, [(local, length), (8, 128)], work(576), moved, side, *rows_all
    )
    objective = total[0, 0] / (length * length)
    return (next_field[None], objective, field_grad[None], forcing_grad)


def fits(initial_field, forcing):
    members, local, length = initial_field.shape
    return (
        members == 1
        and forcing.shape[1] == local
        and forcing.shape[2] == length
        and local == 64
        and length == 32 * local
    )


def per_device(initial_field, target_field, forcing):
    if fits(initial_field, forcing):
        return per_device_fast(initial_field, target_field, forcing)
    return per_device_plain(initial_field, target_field, forcing)


def solution(mesh):
    return jax.shard_map(
        per_device,
        mesh=mesh,
        in_specs=(
            P(None, ("px", "py"), None),
            P(None, ("px", "py"), None),
            P(None, ("px", "py"), None),
        ),
        out_specs=(
            P(None, ("px", "py"), None),
            P(),
            P(None, ("px", "py"), None),
            P(None, ("px", "py"), None),
        ),
        check_vma=False,
    )
```

```python
import math

import jax
import jax.numpy as jnp
import numpy as np
from jax import lax
from jax.experimental import pallas as pl
from jax.experimental.pallas import tpu as pltpu
from jax.sharding import PartitionSpec as P


time_step = 0.25
highest = lax.Precision.HIGHEST


def factor_pair(length):
    first_len = int(math.isqrt(length))
    while length % first_len:
        first_len -= 1
    return (first_len, length // first_len)


def phases(row_count, col_count, period, sign_value, factor):
    product = (
        jnp.arange(row_count, dtype=jnp.int32)[:, None]
        * jnp.arange(col_count, dtype=jnp.int32)[None, :]
        % period
    )
    angles = product.astype(jnp.float32) * (2.0 * math.pi / period)
    return (factor * jnp.cos(angles), sign_value * factor * jnp.sin(angles))


def complex_einsum(formula, left_real, left_imag, table_pair):
    real_term = jnp.einsum(formula, left_real, table_pair[0], precision=highest)
    imag_term = jnp.einsum(formula, left_real, table_pair[1], precision=highest)
    if left_imag is None:
        return (real_term, imag_term)
    real_term = real_term - jnp.einsum(formula, left_imag, table_pair[1], precision=highest)
    imag_term = imag_term + jnp.einsum(formula, left_imag, table_pair[0], precision=highest)
    return (real_term, imag_term)


def transform(real_part, imag_part, sign_value, leading, real_only):
    if leading:
        members, length, span_rows = real_part.shape
        first_len, second_len = factor_pair(length)
        new_shape = (members, first_len, second_len, span_rows)
        formula = "mabr,ak->mrkb"
    else:
        members, span_rows, length = real_part.shape
        first_len, second_len = factor_pair(length)
        new_shape = (members, span_rows, first_len, second_len)
        formula = "mrab,ak->mrkb"
    shaped_real = real_part.reshape(new_shape)
    shaped_imag = None if imag_part is None else imag_part.reshape(new_shape)
    sectioned_out = complex_einsum(
        formula, shaped_real, shaped_imag, phases(first_len, first_len, first_len, sign_value, 1.0)
    )
    twiddle = phases(first_len, second_len, length, sign_value, 1.0 / math.sqrt(length))
    turned_real = sectioned_out[0] * twiddle[0] - sectioned_out[1] * twiddle[1]
    turned_imag = sectioned_out[0] * twiddle[1] + sectioned_out[1] * twiddle[0]
    last_table = phases(second_len, second_len, second_len, sign_value, 1.0)
    final_formula = "mrkb,bq->mrqk"
    if real_only:
        out_real = jnp.einsum(final_formula, turned_real, last_table[0], precision=highest)
        out_real = out_real - jnp.einsum(
            final_formula, turned_imag, last_table[1], precision=highest
        )
        return (out_real.reshape(members, span_rows, length), None)
    out_real, out_imag = complex_einsum(final_formula, turned_real, turned_imag, last_table)
    return (
        out_real.reshape(members, span_rows, length),
        out_imag.reshape(members, span_rows, length),
    )


def regroup(real_part, imag_part):
    moved_real, moved_imag = (
        lax.all_to_all(real_part, ("px", "py"), split_axis=2, concat_axis=1, tiled=True),
        lax.all_to_all(imag_part, ("px", "py"), split_axis=2, concat_axis=1, tiled=True),
    )
    return (moved_real, moved_imag)


def spectral(real_part, imag_part):
    first_pass = transform(real_part, imag_part, -1.0, False, False)
    moved = regroup(first_pass[0], first_pass[1])
    return transform(moved[0], moved[1], -1.0, True, False)


def physical(real_part, imag_part, real_only):
    first_pass = transform(real_part, imag_part, 1.0, False, False)
    moved = regroup(first_pass[0], first_pass[1])
    return transform(moved[0], moved[1], 1.0, True, real_only)


def waves_of(position, count):
    signed = jnp.where(position < count // 2, position, position - count)
    waves = 4.0 * signed.astype(jnp.float32) / count
    derive = jnp.where(position == count // 2, jnp.float32(0.0), waves)
    return (waves, derive)


def per_device_plain(initial_field, target_field, forcing):
    members = initial_field.shape[0]
    full_second = initial_field.shape[2]
    spec_rows = forcing.shape[1]
    full_first = forcing.shape[2]
    device = lax.axis_index(("px", "py"))
    position_first = jnp.arange(full_first, dtype=jnp.int32)
    position_second = device * spec_rows + jnp.arange(spec_rows, dtype=jnp.int32)
    wave_first, deriv_first = waves_of(position_first, full_first)
    wave_second, deriv_second = waves_of(position_second, full_second)
    wave_first = wave_first[None, :]
    deriv_first = deriv_first[None, :]
    wave_second = wave_second[:, None]
    deriv_second = deriv_second[:, None]
    wave_square = wave_first * wave_first + wave_second * wave_second
    denominator = 1.0 + time_step * (wave_square * wave_square - wave_square)
    state_real, state_imag = spectral(initial_field, None)
    slope_real = -deriv_first * state_imag - deriv_second * state_real
    slope_imag = deriv_first * state_real - deriv_second * state_imag
    grad_first, grad_second = physical(slope_real, slope_imag, False)
    nonlinear = -0.5 * (grad_first * grad_first + grad_second * grad_second)
    nonlinear_real, nonlinear_imag = spectral(nonlinear, None)
    next_real = (state_real + time_step * (nonlinear_real + forcing[0])) / denominator
    next_imag = (state_imag + time_step * (nonlinear_imag + forcing[1])) / denominator
    next_field, _ = physical(next_real, next_imag, True)
    residual = next_field - target_field
    total = lax.psum(0.5 * jnp.sum(residual * residual), ("px", "py"))
    objective = total / (members * full_first * full_second)
    misfit_real, misfit_imag = spectral(residual, None)
    coef_real = misfit_real / denominator
    coef_imag = misfit_imag / denominator
    forcing_grad = time_step * jnp.stack([jnp.sum(coef_real, axis=0), jnp.sum(coef_imag, axis=0)])
    multiplier, _ = physical(time_step * coef_real, time_step * coef_imag, True)
    joint_real, joint_imag = spectral(multiplier * grad_first, multiplier * grad_second)
    total_real = coef_real - deriv_first * joint_imag + deriv_second * joint_real
    total_imag = coef_imag + deriv_first * joint_real + deriv_second * joint_imag
    field_grad, _ = physical(total_real, total_imag, True)
    return (next_field, objective, field_grad, forcing_grad)


def split_of(value):
    high = value.astype(jnp.bfloat16)
    low = (value - high.astype(jnp.float32)).astype(jnp.bfloat16)
    return high, low


def dots(high, low, table_high, table_low):
    def one(left, right):
        return jnp.dot(left, right, preferred_element_type=jnp.float32)

    return one(high, table_high) + (one(low, table_high) + one(high, table_low))


def turn(pair, cosine, sine):
    real, imag = pair
    return real * cosine - imag * sine, imag * cosine + real * sine


def butterflies(values, sign):
    count = len(values)
    if count == 1:
        return values
    even = butterflies(values[0::2], sign)
    odd = butterflies(values[1::2], sign)
    half = count // 2
    first, second = [], []
    root = math.sqrt(0.5)
    for place in range(half):
        real, imag = odd[place]
        if place == 0:
            turned = (real, imag)
        elif 4 * place == count:
            turned = (-sign * imag, sign * real)
        elif 8 * place == count:
            turned = (root * (real - sign * imag), root * (imag + sign * real))
        elif 8 * place == 3 * count:
            turned = (root * (-real - sign * imag), root * (sign * real - imag))
        else:
            angle = 2.0 * math.pi * place / count
            turned = turn((real, imag), math.cos(angle), sign * math.sin(angle))
        base_real, base_imag = even[place]
        first.append((base_real + turned[0], base_imag + turned[1]))
        second.append((base_real - turned[0], base_imag - turned[1]))
    return first + second


def np_split(table):
    high = np.asarray(table, np.float32).astype(jnp.bfloat16)
    low = (np.asarray(table, np.float64) - high.astype(np.float64)).astype(jnp.bfloat16)
    return jnp.asarray(high), jnp.asarray(low)


class Tables:
    def __init__(self, length, parts):
        radix = 8
        inner = length // radix
        lanes = length // parts
        scale = 1.0 / math.sqrt(length)
        spot = np.arange(inner)
        angle = 2.0 * np.pi * (np.outer(spot, spot) % inner) / inner
        self.row_pair = np_split(scale * np.concatenate([np.cos(angle), np.sin(angle)], 1))
        classes = np.arange(radix)
        angle = 2.0 * np.pi * np.outer(classes, spot) / length
        self.row_turn = (
            jnp.asarray(np.cos(angle), jnp.float32),
            jnp.asarray(np.sin(angle), jnp.float32),
        )
        half = inner // 2
        place = np.arange(lanes)
        angle = 2.0 * np.pi * (np.outer(place, place) % lanes) / lanes
        eye = np.eye(inner // lanes)
        self.col_pair = np_split(
            scale * np.concatenate([np.kron(eye, np.cos(angle)), np.kron(eye, np.sin(angle))], 1)
        )
        outer = np.arange(parts)
        angle = 2.0 * np.pi * np.outer(outer, np.tile(place, inner // lanes)) / length
        self.col_turn = (
            jnp.asarray(np.cos(angle), jnp.float32),
            jnp.asarray(np.sin(angle), jnp.float32),
        )
        index = outer[:, None] + parts * np.tile(place, inner // lanes)[None, :]
        signed = np.where(index < length // 2, index, index - length)
        waves = 4.0 * signed / length
        self.col_wave = waves
        self.col_deriv = jnp.asarray(np.where(index == length // 2, 0.0, waves), jnp.float32)
        index = np.stack([radix * spot + one for one in range(4)])
        index[0, half:] += 4
        signed = np.where(index < length // 2, index, index - length)
        waves = 4.0 * signed / length
        waves[0, 0] = 0.0
        self.row_deriv = jnp.asarray(waves, jnp.float32)


def eight_real(blocks):
    plus = [blocks[i] + blocks[i + 4] for i in range(4)]
    minus = [blocks[i] - blocks[i + 4] for i in range(4)]
    root = math.sqrt(0.5)
    even, odd = plus[0] + plus[2], plus[1] + plus[3]
    near, far = root * (minus[1] - minus[3]), root * (minus[1] + minus[3])
    return {
        0: even + odd,
        4: even - odd,
        1: (minus[0] + near, -minus[2] - far),
        2: (plus[0] - plus[2], plus[3] - plus[1]),
        3: (minus[0] - near, minus[2] - far),
    }


def rows_forward(load, high, low, product, pair, spin, other):
    for row in range(0, 64, 16):
        for lane in range(0, 256, 128):
            rows, lanes = slice(row, row + 16), slice(lane, lane + 128)
            mixed = eight_real([load(one, rows, lanes) for one in range(8)])

            def spun(kind, real, imag):
                cosine = spin[0][kind : kind + 1, lanes]
                sine = spin[1][kind : kind + 1, lanes]
                if imag is None:
                    return real * cosine, -real * sine
                return real * cosine + imag * sine, imag * cosine - real * sine

            out = [None] * 9
            out[0] = mixed[0]
            for one in (1, 2, 3):
                if other:
                    real, imag = mixed[4 - one]
                    out[one], out[3 + one] = spun(4 + one, real, -imag)
                else:
                    out[one], out[3 + one] = spun(one, *mixed[one])
            out[7], out[8] = spun(4, mixed[4], None)
            for place in range(9):
                top, bottom = split_of(out[place])
                at = slice(64 * place + row, 64 * place + row + 16)
                high[at, lanes] = top
                low[at, lanes] = bottom
    product[0:576, :] = dots(high[0:576, :], low[0:576, :], pair[0][...], pair[1][...])

    def cosine(place, lanes=slice(0, 256)):
        return product[64 * place : 64 * place + 64, lanes]

    def sine(place, lanes=slice(0, 256)):
        moved = slice(lanes.start + 256, lanes.stop + 256)
        return product[64 * place : 64 * place + 64, moved]

    front, back = slice(0, 128), slice(128, 256)
    if other:
        real = [jnp.concatenate([cosine(7, front) + sine(8, front), cosine(0, back)], 1)]
        imag = [jnp.concatenate([cosine(8, front) - sine(7, front), -sine(0, back)], 1)]
    else:
        lane = lax.broadcasted_iota(jnp.int32, (64, 128), 1)
        first = jnp.where(lane == 0, cosine(0, back), -sine(0, front))
        real = [jnp.concatenate([cosine(0, front), cosine(7, back) + sine(8, back)], 1)]
        imag = [jnp.concatenate([first, cosine(8, back) - sine(7, back)], 1)]
    for one in (1, 2, 3):
        real.append(cosine(one) + sine(3 + one))
        imag.append(cosine(3 + one) - sine(one))
    return real + imag


def rows_store(slots, target, offset):
    for place in range(0, 8, 2):
        both = jnp.concatenate([slots[place], slots[place + 1]], 0)
        target[:, :, offset + 64 * place : offset + 64 * place + 128] = both.T.reshape(32, 8, 128)


def rows_derived(slots, deriv):
    out = [None] * 8
    for one in range(4):
        wave = deriv[one : one + 1, :]
        out[one] = -wave * slots[4 + one]
        out[4 + one] = wave * slots[one]
    return out


def rows_loaded(source, offset):
    out = []
    for place in range(0, 8, 2):
        both = source[:, :, offset + 64 * place : offset + 64 * place + 128]
        both = both.reshape(256, 128).T
        out += [both[:64], both[64:]]
    return out


def put(high, low, place, value):
    top, bottom = split_of(value)
    high[64 * place : 64 * place + 64, :] = top
    low[64 * place : 64 * place + 64, :] = bottom


def eight_inverse(even, odd, ones, twos, threes, store):
    root = math.sqrt(0.5)
    plus, minus = even + odd, even - odd
    back = root * (ones[0] - ones[1]) - root * (threes[0] + threes[1])
    fore = root * (threes[0] - threes[1]) - root * (ones[0] + ones[1])
    parts = (
        (plus + twos[0], ones[0] + threes[0]),
        (minus - twos[1], back),
        (plus - twos[0], threes[1] - ones[1]),
        (minus + twos[1], fore),
    )
    for one in range(4):
        store(one, parts[one][0] + parts[one][1])
        store(one + 4, parts[one][0] - parts[one][1])


def rows_inverse(slots, high, low, product, pair, spin, store):
    for one in (1, 2, 3):
        put(high, low, one - 1, slots[one])
        put(high, low, 2 + one, slots[4 + one])
    front, back = slice(0, 128), slice(128, 256)
    real, imag = slots[0], slots[4]
    first = lax.broadcasted_iota(jnp.int32, (64, 128), 1) == 0
    none = jnp.zeros((64, 128), jnp.float32)
    real_front = jnp.where(first, 0.5 * real[:, front], real[:, front])
    imag_front = jnp.where(first, 0.0, imag[:, front])
    middle = jnp.where(first, 0.5 * imag[:, front], 0.0)
    put(high, low, 6, jnp.concatenate([real_front, middle], 1))
    put(high, low, 7, jnp.concatenate([imag_front, none], 1))
    put(high, low, 8, jnp.concatenate([none, real[:, back]], 1))
    put(high, low, 9, jnp.concatenate([none, imag[:, back]], 1))
    product[0:640, :] = dots(high[0:640, :], low[0:640, :], pair[0][...], pair[1][...])
    for row in range(0, 64, 16):
        for lane in range(0, 256, 128):
            lanes, moved = slice(lane, lane + 128), slice(lane + 256, lane + 384)

            def mixed(real_place, imag_place):
                at = slice(64 * real_place + row, 64 * real_place + row + 16)
                to = slice(64 * imag_place + row, 64 * imag_place + row + 16)
                return (
                    product[at, lanes] - product[to, moved],
                    product[to, lanes] + product[at, moved],
                )

            def spun(one, real_place, imag_place):
                return turn(
                    mixed(real_place, imag_place),
                    2.0 * spin[0][one : one + 1, lanes],
                    2.0 * spin[1][one : one + 1, lanes],
                )

            turned = [spun(one, one - 1, 2 + one) for one in (1, 2, 3)]
            eight_inverse(
                2.0 * mixed(6, 7)[0],
                spun(4, 8, 9)[0],
                *turned,
                lambda one, value: store(one, slice(row, row + 16), slice(lane, lane + 128), value),
            )


def put_tiles(high, low, place, first, second, lanes):
    top, bottom = split_of(jnp.concatenate([first, second], 0))
    high[8 * place : 8 * place + 16, lanes] = top
    low[8 * place : 8 * place + 16, lanes] = bottom


def cols_forward(source, offset, high, low, product, pair, spin):
    for lane in range(0, 256, 128):
        lanes = slice(lane, lane + 128)
        values = [
            (
                source[one, :, offset + lane : offset + lane + 128],
                source[one, :, offset + 256 + lane : offset + 384 + lane],
            )
            for one in range(32)
        ]
        values = butterflies(values, -1)
        for one in range(32):
            values[one] = turn(
                values[one], spin[0][one : one + 1, lanes], -spin[1][one : one + 1, lanes]
            )
        for one in range(0, 32, 2):
            put_tiles(high, low, one, values[one][0], values[one + 1][0], lanes)
            put_tiles(high, low, 32 + one, values[one][1], values[one + 1][1], lanes)
    product[0:512, :] = dots(high[0:512, :], low[0:512, :], pair[0][...], pair[1][...])

    def tile(one, lanes=slice(0, 256)):
        at, to = slice(8 * one, 8 * one + 8), slice(256 + 8 * one, 264 + 8 * one)
        moved = slice(lanes.start + 256, lanes.stop + 256)
        return (
            product[at, lanes] + product[to, moved],
            product[to, lanes] - product[at, moved],
        )

    return tile


def cols_inverse(tile, high, low, product, pair, spin, targets, offset):
    for group, target in enumerate(targets):
        for one in range(0, 32, 2):
            first, second = tile(one, group), tile(one + 1, group)
            put_tiles(high, low, one, first[0], second[0], slice(0, 256))
            put_tiles(high, low, 32 + one, first[1], second[1], slice(0, 256))
        product[0:512, :] = dots(high[0:512, :], low[0:512, :], pair[0][...], pair[1][...])
        for lane in range(0, 256, 128):
            lanes, moved = slice(lane, lane + 128), slice(lane + 256, lane + 384)
            values = []
            for one in range(32):
                at, to = slice(8 * one, 8 * one + 8), slice(256 + 8 * one, 264 + 8 * one)
                value = (
                    product[at, lanes] - product[to, moved],
                    product[to, lanes] + product[at, moved],
                )
                values.append(
                    turn(value, spin[0][one : one + 1, lanes], spin[1][one : one + 1, lanes])
                )
            values = butterflies(values, 1)
            for one in range(32):
                at = offset + lane
                target[one, :, at : at + 128] = values[one][0]
                at += 256
                target[one, :, at : at + 128] = values[one][1]


def mirrored(tile, one):
    real, imag = tile((32 - one) % 32)
    lane = lax.broadcasted_iota(jnp.int32, (8, 128), 1)
    spot = jnp.where(lane < 64, (64 - lane) % 64 if one == 0 else 63 - lane, lane)
    return (
        jnp.take_along_axis(real, spot, axis=1),
        -jnp.take_along_axis(imag, spot, axis=1),
    )


def kernel_start(field, ph, pl_, sc, ss, out, high, low, product):
    def load(one, rows, lanes):
        return field[rows, 256 * one + lanes.start : 256 * one + lanes.stop]

    slots = rows_forward(load, high, low, product, (ph, pl_), (sc, ss), False)
    rows_store(slots, out, 0)


def kernel_slope(field, ph, pl_, sc, ss, deriv, out, high, low, product):
    def load(one, rows, lanes):
        return field[rows, 256 * one + lanes.start : 256 * one + lanes.stop]

    def store(one, rows, lanes, value):
        out[rows, 256 * one + lanes.start : 256 * one + lanes.stop] = value

    slots = rows_forward(load, high, low, product, (ph, pl_), (sc, ss), False)
    slots = rows_derived(slots, deriv)
    rows_inverse(
        slots, high, low, product, (ph, pl_), (sc, ss), store
    )


def kernel_force(
    place, force, ch, cl, tc, ts,
    own, far_one, far_two, corner, mixed, back, turned, spec, far, high, low, product,
):
    early = place[0] < 16
    for lane in range(0, 2048, 128):
        both = jnp.concatenate([force[part, :, lane : lane + 128] for part in range(2)], 0)
        turned[lane : lane + 128, :] = both.T
    lane = lax.broadcasted_iota(jnp.int32, (8, 128), 1)
    for one in range(0, 32, 2):
        both = jnp.concatenate(
            [turned[pl.ds(one, 64, stride=32), :], turned[pl.ds(one + 1, 64, stride=32), :]], 0
        ).T
        base, base_back = 64 * one, 72 * one
        mixed[base : base + 128, :] = both
        for part in range(2):
            start = base_back + 72 * part
            back[start : start + 8, :] = both[64 * part : 64 * part + 8]
            for row in range(8):
                at = start + 64 - 8 * row
                back[at : at + 8, :] = both[64 * part + 8 * row : 64 * part + 8 * row + 8]
            at = base + 64 * part

            def rising(kind):
                return mixed[pl.ds(at + kind, 8, stride=8), :]

            def falling(kind):
                return back[pl.ds(start + 8 + kind, 8, stride=8), :]

            slots = [jnp.where(early, rising(0), rising(4))]
            slots += [rising(kind) for kind in (1, 2, 3)]
            around = back[pl.ds(start, 8, stride=8), :]
            slots += [jnp.where(early, falling(4), around)]
            slots += [falling(kind) for kind in (7, 6, 5)]
            for slot in range(0, 8, 2):
                first, second = slots[slot], slots[slot + 1]
                lanes = slice(512 * part + 64 * slot, 512 * part + 64 * slot + 128)
                spec[8 * one : 8 * one + 8, lanes] = jnp.where(
                    lane < 64, first, pltpu.roll(second, 64, 1)
                )
                spec[8 * one + 8 : 8 * one + 16, lanes] = jnp.where(
                    lane < 64, pltpu.roll(first, 64, 1), second
                )

    def tile(one, group):
        rows = slice(8 * one, 8 * one + 8)
        return (
            spec[rows, 256 * group : 256 * group + 256],
            spec[rows, 512 + 256 * group : 768 + 256 * group],
        )

    cols_inverse(tile, high, low, product, (ch, cl), (tc, ts), [own, far], 0)
    for one in range(32):
        corner[one : one + 1, :] = far[one, 0:1, :]
    far_one[...] = far[0:16]
    far_two[...] = far[16:32]


def kernel_merge(
    place, own, far_one, far_two, corner, state, ch, cl, tc, ts, out, joint, high, low, product
):
    row = lax.broadcasted_iota(jnp.int32, (8, 128), 0)
    lane = lax.broadcasted_iota(jnp.int32, (8, 128), 1)
    edge = jnp.logical_and(row == 0, lane < 64)
    fixed = jnp.logical_and(edge, place[0] < 16)
    packed = jnp.logical_and(edge, place[0] == 0)
    for one in range(32):
        far, at = (far_one, one) if one < 16 else (far_two, one - 16)
        for start in range(0, 256, 128):
            lanes, moved = slice(start, start + 128), slice(start + 256, start + 384)
            own_real, own_imag = own[one, :, lanes], own[one, :, moved]
            far_real, far_imag = far[at, :, lanes], far[at, :, moved]
            if start == 0:
                far_real = jnp.where(fixed, corner[one : one + 1, lanes], far_real)
                far_imag = jnp.where(fixed, corner[one : one + 1, moved], far_imag)
            real, imag = 0.5 * (own_real + far_real), 0.5 * (own_imag - far_imag)
            if start == 0:
                real = jnp.where(packed, own_real, real)
                imag = jnp.where(packed, far_real, imag)
            joint[one, :, lanes] = real
            joint[one, :, moved] = imag
    tile = cols_forward(joint, 0, high, low, product, (ch, cl), (tc, ts))
    for one in range(32):
        rows = slice(8 * one, 8 * one + 8)
        real, imag = tile(one)
        out[0, rows, :] = state[0, rows, :] + time_step * real
        out[1, rows, :] = state[1, rows, :] + time_step * imag


def kernel_first(source, ahead, ch, cl, tc, ts, deriv, state, out, high, low, product):
    tile = cols_forward(source, 0, high, low, product, (ch, cl), (tc, ts))
    for one in range(32):
        rows = slice(8 * one, 8 * one + 8)
        real, imag = tile(one)
        state[0, rows, :] = real
        state[1, rows, :] = imag
    state.send()

    def slope(one, group):
        rows = slice(8 * one, 8 * one + 8)
        wave = deriv[one : one + 1, :]
        return -wave * state[1, rows, :], wave * state[0, rows, :]

    cols_inverse(slope, high, low, product, (ch, cl), (tc, ts), [out], 0)


def kernel_bend(
    source, second, other, ph, pl_, sc, ss, grad, out, bend, high, low, product
):
    def store(one, rows, lanes, value):
        to = slice(256 * one + lanes.start, 256 * one + lanes.stop)
        grad[rows, to] = value
        side = second[rows, to]
        bend[rows, to] = -0.5 * (value * value + side * side)

    slots = rows_loaded(source, 0)
    rows_inverse(slots, high, low, product, (ph, pl_), (sc, ss), store)
    grad.send()

    def load(one, rows, lanes):
        return bend[rows, 256 * one + lanes.start : 256 * one + lanes.stop]

    slots = rows_forward(load, high, low, product, (ph, pl_), (sc, ss), False)
    rows_store(slots, out, 0)
    out[:, :, 512:1024] = other[...]


def kernel_solve(
    source, state, damp, cross, ch, cl, tc, ts, coef, out, goal, fresh, high, low, product
):
    tile = cols_forward(source, 512, high, low, product, (ch, cl), (tc, ts))
    for one in range(32):
        rows = slice(8 * one, 8 * one + 8)
        goal[0, rows, :], goal[1, rows, :] = tile(one)
    tile = cols_forward(source, 0, high, low, product, (ch, cl), (tc, ts))
    for one in range(32):
        rows = slice(8 * one, 8 * one + 8)
        real, imag = tile(one)
        fresh[0, rows, :] = state[0, rows, :] + time_step * real
        fresh[1, rows, :] = state[1, rows, :] + time_step * imag

    def front(array):
        def view(one):
            rows = slice(8 * one, 8 * one + 8)
            return array[0, rows, 0:128], array[1, rows, 0:128]

        return view

    def damped(value, flipped, one):
        rows = slice(8 * one, 8 * one + 8)
        weight, mixed = damp[rows, :], cross[rows, :]
        return tuple(
            jnp.concatenate(
                [
                    value[part][:, 0:128] * weight[:, 0:128] + flipped[part] * mixed,
                    value[part][:, 128:256] * weight[:, 128:256],
                ],
                1,
            )
            for part in range(2)
        )

    for one in range(32):
        rows = slice(8 * one, 8 * one + 8)
        value = (fresh[0, rows, :], fresh[1, rows, :])
        flipped = mirrored(front(fresh), one)
        following = damped(value, flipped, one)
        weight, mixed = damp[rows, 0:128], cross[rows, :]
        back = mirrored(front(goal), one)
        turned_back = tuple(
            flipped[part] * weight + value[part][:, 0:128] * mixed - back[part]
            for part in range(2)
        )
        miss = tuple(following[part] - goal[part, rows, :] for part in range(2))
        slope = damped(miss, turned_back, one)
        for part in range(2):
            coef[part, rows, :] = time_step * slope[part]
            goal_next = following[part]
            product[256 * part + 8 * one : 256 * part + 8 * one + 8, 0:256] = goal_next
    coef.send()
    for part in range(2):
        fresh[part, :, :] = product[256 * part : 256 * part + 256, 0:256]

    def scaled(one, group):
        rows = slice(8 * one, 8 * one + 8)
        return coef[0, rows, :], coef[1, rows, :]

    def following_tile(one, group):
        rows = slice(8 * one, 8 * one + 8)
        return fresh[0, rows, :], fresh[1, rows, :]

    cols_inverse(scaled, high, low, product, (ch, cl), (tc, ts), [out], 0)
    cols_inverse(following_tile, high, low, product, (ch, cl), (tc, ts), [out], 512)


def kernel_adjoint(
    source, grad, ph, pl_, sc, ss, mult, out, joint, high, low, product
):
    def store(one, rows, lanes, value):
        to = slice(256 * one + lanes.start, 256 * one + lanes.stop)
        mult[rows, to] = value
        joint[rows, to] = value * grad[rows, to]

    slots = rows_loaded(source, 0)
    rows_inverse(slots, high, low, product, (ph, pl_), (sc, ss), store)
    mult.send()

    def load(one, rows, lanes):
        return joint[rows, 256 * one + lanes.start : 256 * one + lanes.stop]

    slots = rows_forward(load, high, low, product, (ph, pl_), (sc, ss), False)
    rows_store(slots, out, 0)

    def load_other(one, rows, lanes):
        return mult[rows, 256 * one + lanes.start : 256 * one + lanes.stop]

    slots = rows_forward(load_other, high, low, product, (ph, pl_), (sc, ss), True)
    rows_store(slots, out, 512)


def kernel_side(
    source, goal, mult, second, ph, pl_, sc, ss, deriv,
    ahead, side, miss, joint, high, low, product,
):
    def store(one, rows, lanes, value):
        to = slice(256 * one + lanes.start, 256 * one + lanes.stop)
        ahead[rows, to] = value
        joint[rows, to] = mult[rows, to] * second[rows, to]

    slots = rows_loaded(source, 512)
    rows_inverse(slots, high, low, product, (ph, pl_), (sc, ss), store)
    total = jnp.zeros((8, 256), jnp.float32)
    for row in range(0, 64, 8):
        for lane in range(0, 2048, 256):
            gap = ahead[row : row + 8, lane : lane + 256] - goal[row : row + 8, lane : lane + 256]
            total = total + gap * gap
    miss[...] = jnp.broadcast_to(0.5 * jnp.sum(total), (8, 128))

    def load(one, rows, lanes):
        return joint[rows, 256 * one + lanes.start : 256 * one + lanes.stop]

    slots = rows_forward(load, high, low, product, (ph, pl_), (sc, ss), False)
    slots = rows_derived(slots, deriv)
    for place in range(8):
        side[64 * place : 64 * place + 64, :] = slots[place]


def kernel_last(source, coef, miss, ch, cl, tc, ts, deriv, out, spec, high, low, product):
    tile = cols_forward(source, 0, high, low, product, (ch, cl), (tc, ts))
    for one in range(32):
        rows = slice(8 * one, 8 * one + 8)
        real, imag = tile(one)
        wave = deriv[one : one + 1, :]
        spec[0, rows, :] = coef[0, rows, :] * (1.0 / time_step) - wave * imag
        spec[1, rows, :] = coef[1, rows, :] * (1.0 / time_step) + wave * real

    def whole(one, group):
        rows = slice(8 * one, 8 * one + 8)
        return spec[0, rows, :], spec[1, rows, :]

    cols_inverse(whole, high, low, product, (ch, cl), (tc, ts), [out], 0)
    out[:, :, 512:640] = jnp.broadcast_to(miss[...][None], (32, 8, 128))


def kernel_force_grad(
    place, source, coef, ch, cl, tc, ts, out, mixed, turned, high, low, product
):
    tile = cols_forward(source, 512, high, low, product, (ch, cl), (tc, ts))
    early = place[0] < 16
    corner = place[0] == 0
    lane = lax.broadcasted_iota(jnp.int32, (8, 128), 1)
    row = lax.broadcasted_iota(jnp.int32, (8, 128), 0)
    packed = jnp.logical_and(jnp.logical_and(row == 0, lane < 64), corner)

    def front(one):
        rows = slice(8 * one, 8 * one + 8)
        return coef[0, rows, 0:128], coef[1, rows, 0:128]

    def lanes_of(one):
        rows = slice(8 * one, 8 * one + 8)
        far = tile(one)
        flipped = mirrored(front, one)
        out_parts = []
        for part in range(2):
            near_front = coef[part, rows, 0:128]
            near_front = jnp.where(packed, 0.5 * (near_front + flipped[part]), near_front)
            near_back = coef[part, rows, 128:256]
            far_front, far_back = far[part][:, 0:128], far[part][:, 128:256]
            low_half = lane < 64
            swap = jnp.logical_and(low_half, jnp.logical_not(early))
            out_parts.append(
                [
                    jnp.where(swap, far_front, near_front),
                    near_back,
                    jnp.where(swap, near_front, far_front),
                    far_back,
                ]
            )
        return out_parts

    for one in range(0, 32, 2):
        first, second = lanes_of(one), lanes_of(one + 1)
        base = 64 * one
        for part in range(2):
            for pairs in range(4):
                left, right = first[part][pairs], second[part][pairs]
                at = base + 64 * part + 2 * pairs
                mixed[pl.ds(at, 8, stride=8), :] = jnp.where(
                    lane < 64, left, pltpu.roll(right, 64, 1)
                )
                mixed[pl.ds(at + 1, 8, stride=8), :] = jnp.where(
                    lane < 64, pltpu.roll(left, 64, 1), right
                )
        both = mixed[base : base + 128, :].T
        turned[pl.ds(one, 64, stride=32), :] = both[:64]
        turned[pl.ds(one + 1, 64, stride=32), :] = both[64:]
    for start in range(0, 2048, 128):
        both = turned[start : start + 128, :].T
        for part in range(2):
            out[part, :, start : start + 128] = both[64 * part : 64 * part + 64]


def kernel_finish(source, side, ph, pl_, sc, ss, out, total, high, low, product):
    slots = rows_loaded(source, 0)
    slots = [slots[place] + side[64 * place : 64 * place + 64, :] for place in range(8)]

    def store(one, rows, lanes, value):
        out[rows, 256 * one + lanes.start : 256 * one + lanes.stop] = value

    rows_inverse(slots, high, low, product, (ph, pl_), (sc, ss), store)
    total[0, 0] = jnp.sum(source[:, 0:1, 512:640]) * (1.0 / (128.0 * out.formed.shape[1] ** 2))


class Leaving:
    def __init__(self, formed, copy):
        self.formed, self.copy, self.gone = formed, copy, False

    def send(self):
        if not self.gone:
            self.copy.start()
            self.gone = True

    def __getitem__(self, index):
        return self.formed[index]

    def __setitem__(self, index, value):
        self.formed[index] = value


def call(body, outputs, scratch, *operands, scalars=0, near=0, number=False):
    lead_count = scalars + near
    fields = operands[lead_count:]
    count, made = len(fields), len(outputs)

    def whole(*refs):
        lead, refs = refs[:lead_count], refs[lead_count:]
        given, results, refs = refs[:count], refs[count : count + made], refs[count + made :]
        last, refs = (refs[:1], refs[1:]) if number else ((), refs)
        held, formed, refs = refs[:count], refs[count : count + made], refs[count + made :]
        extra, into, onto = refs[:-2], refs[-2], refs[-1]
        arrivals = [
            pltpu.make_async_copy(given[one], held[one], into.at[one]) for one in range(count)
        ]
        for one in arrivals:
            one.start()
        departures = [
            Leaving(formed[one], pltpu.make_async_copy(formed[one], results[one], onto.at[one]))
            for one in range(made)
        ]
        for one in arrivals:
            one.wait()
        body(*lead, *held, *departures, *last, *extra)
        for one in departures:
            one.send()
        for one in departures:
            one.copy.wait()

    specs = [pl.BlockSpec(memory_space=pltpu.SMEM)] * scalars
    specs += [pl.BlockSpec(memory_space=pltpu.VMEM)] * near
    specs += [pl.BlockSpec(memory_space=pltpu.HBM)] * count
    scratch = (
        [pltpu.VMEM(one.shape, one.dtype) for one in fields]
        + [pltpu.VMEM(one, jnp.float32) for one in outputs]
        + scratch
        + [pltpu.SemaphoreType.DMA((count,)), pltpu.SemaphoreType.DMA((made,))]
    )
    return pl.pallas_call(
        whole,
        out_shape=tuple(pltpu.HBM(one, jnp.float32) for one in outputs)
        + (jax.ShapeDtypeStruct((1, 1), jnp.float32),) * number,
        in_specs=specs,
        out_specs=tuple(pl.BlockSpec(memory_space=pltpu.HBM) for _ in outputs)
        + (pl.BlockSpec(memory_space=pltpu.SMEM),) * number,
        scratch_shapes=scratch,
        compiler_params=pltpu.CompilerParams(vmem_limit_bytes=24 * 2**20),
    )(*operands[:lead_count], *[pltpu.with_memory_space_constraint(one, pltpu.HBM) for one in fields])


def work(rows):
    return [
        pltpu.VMEM((rows, 256), jnp.bfloat16),
        pltpu.VMEM((rows, 256), jnp.bfloat16),
        pltpu.VMEM((rows, 512), jnp.float32),
    ]


def exchange(value):
    return lax.all_to_all(value, ("px", "py"), split_axis=0, concat_axis=0, tiled=True)


def per_device_fast(initial_field, target_field, forcing):
    length = initial_field.shape[2]
    local = initial_field.shape[1]
    parts = length // local
    device = lax.axis_index(("px", "py"))
    tables = Tables(length, parts)
    inner = length // 8
    field, goal = initial_field[0], target_field[0]
    rows = tables.row_pair + tables.row_turn
    cols = tables.col_pair + tables.col_turn
    f32 = jnp.float32
    own = jnp.arange(8, dtype=jnp.int32)[None, :, None]
    kind = jnp.arange(inner, dtype=jnp.int32)[None, None, :] // local
    late = jnp.where(device < parts // 2, 0, 4)
    second = device * local + 8 * own + jnp.where(kind == 0, late, kind)
    wave_first = jnp.asarray(tables.col_wave, f32)[:, None, :]

    def inverse_of(index):
        wave = waves_of(index, length)[0]
        square = wave_first * wave_first + wave * wave
        return 1.0 / (1.0 + time_step * (square * square - square))

    packed = (second == 0) & (kind == 0)
    plain = inverse_of(second)
    middle = inverse_of(second + length // 2)
    damp = jnp.where(packed, 0.5 * (plain + middle), plain).reshape(inner, inner)
    cross = jnp.where(packed, 0.5 * (plain - middle), 0.0).reshape(inner, inner)[:, :128]

    block = (parts, 8, 512)
    (sent,) = call(kernel_start, [block], work(640), field, *rows)
    first = exchange(sent)
    spot = jnp.asarray(device, jnp.int32).reshape(1)
    half_block = (parts // 2, 8, 512)
    own_force, far_one, far_two, corner_own = call(
        kernel_force,
        [block, half_block, half_block, (parts, 512)],
        [
            pltpu.VMEM((length, 128), f32),
            pltpu.VMEM((length + 256, 128), f32),
            pltpu.VMEM((length, 128), f32),
            pltpu.VMEM((256, 1024), f32),
            pltpu.VMEM(block, f32),
        ]
        + work(512),
        spot,
        forcing,
        *cols,
        scalars=1,
    )
    middle_part = parts // 2
    mirror = [(one, parts - 1 - one) for one in range(parts)]
    around = [(middle_part, 0)]
    around += [(middle_part + one, middle_part - one) for one in range(1, middle_part)]
    far_one = lax.ppermute(far_one, ("px", "py"), mirror)
    far_two = lax.ppermute(far_two, ("px", "py"), mirror)
    corner = lax.ppermute(corner_own, ("px", "py"), around)
    (goal_rows,) = call(kernel_start, [block], work(640), goal, *rows)
    (grad_second,) = call(
        kernel_slope, [(local, length)], work(640), field, *rows, tables.row_deriv
    )
    state, sent = call(
        kernel_first,
        [(2, 256, 256), block],
        work(512),
        first,
        corner_own,
        *cols,
        tables.col_deriv,
        near=1,
    )
    moved = exchange(sent)
    grad_first, sent = call(
        kernel_bend,
        [(local, length), (parts, 8, 1024)],
        [pltpu.VMEM((local, length), f32)] + work(640),
        moved,
        grad_second,
        goal_rows,
        *rows,
        near=1,
    )
    moved = exchange(sent)
    (state,) = call(
        kernel_merge,
        [(2, 256, 256)],
        [pltpu.VMEM(block, f32)] + work(512),
        spot,
        own_force,
        far_one,
        far_two,
        corner,
        state,
        *cols,
        scalars=1,
    )
    coef, sent = call(
        kernel_solve,
        [(2, 256, 256), (parts, 8, 1024)],
        [pltpu.VMEM((2, 256, 256), f32), pltpu.VMEM((2, 256, 256), f32)] + work(512),
        moved,
        state,
        damp,
        cross,
        *cols,
        near=1,
    )
    moved = exchange(sent)
    mult, sent = call(
        kernel_adjoint,
        [(local, length), (parts, 8, 1024)],
        [pltpu.VMEM((local, length), f32)] + work(640),
        moved,
        grad_first,
        *rows,
        near=1,
    )
    next_field, side, miss = call(
        kernel_side,
        [(local, length), (512, 256), (8, 128)],
        [pltpu.VMEM((local, length), f32)] + work(640),
        moved,
        goal,
        mult,
        grad_second,
        *rows,
        tables.row_deriv,
    )
    moved = exchange(sent)
    (sent,) = call(
        kernel_last,
        [(parts, 8, 640)],
        [pltpu.VMEM((2, 256, 256), f32)] + work(512),
        moved,
        coef,
        miss,
        *cols,
        tables.col_deriv,
        near=1,
    )
    (forcing_grad,) = call(
        kernel_force_grad,
        [(2, local, length)],
        [pltpu.VMEM((length, 128), f32), pltpu.VMEM((length, 128), f32)] + work(512),
        spot,
        moved,
        coef,
        *cols,
        scalars=1,
    )
    moved = exchange(sent)
    field_grad, total = call(
        kernel_finish, [(local, length)], work(640), moved, side, *rows, near=1, number=True
    )
    objective = total.reshape(())
    return (next_field[None], objective, field_grad[None], forcing_grad)


def fits(initial_field, forcing):
    members, local, length = initial_field.shape
    return (
        members == 1
        and forcing.shape[1] == local
        and forcing.shape[2] == length
        and local == 64
        and length == 32 * local
    )


def per_device(initial_field, target_field, forcing):
    if fits(initial_field, forcing):
        return per_device_fast(initial_field, target_field, forcing)
    return per_device_plain(initial_field, target_field, forcing)


def solution(mesh):
    return jax.shard_map(
        per_device,
        mesh=mesh,
        in_specs=(
            P(None, ("px", "py"), None),
            P(None, ("px", "py"), None),
            P(None, ("px", "py"), None),
        ),
        out_specs=(
            P(None, ("px", "py"), None),
            P(),
            P(None, ("px", "py"), None),
            P(None, ("px", "py"), None),
        ),
        check_vma=False,
    )
```
